32 devices in a mesh: row: 4 (over y, x), col: 8 (over z, core).
Axes of the slice: x: 2, y: 2, z: 4, core: 2. Of those that a mesh axis runs over, the one named last changes fastest.
Arguments:
- grad_out: bfloat16 [512, 8192], P('col', 'row'), may hold values from -6 to 6
- weight: bfloat16 [28672, 8192], P('col', 'row'), may hold values from -0.0625 to 0.0625
Outputs:
- grad_in: bfloat16 [512, 28672], P('row', 'col')
The draws below stay inside these ranges and needn't reach their ends.
All inputs are finite; a program needn't handle non-finite values.
Results may differ from the reference program's by a relative error of at most 0.001.
Values may be sent and summed in bfloat16 or wider, within the bound.
No kernel may reach another device: no remote copies, remote signals or barrier semaphores. Data moves between devices by JAX's collectives and lax.ppermute only.
A program may use at most 64 MiB of HBM per device.

```python
import jax
import jax.numpy as jnp
from jax import lax

D = 8192
FF = 28672
TOKENS = 512


def with_spikes(array, key, source, target, parts, factor):
    def block_of(axis_at):
        return (jnp.arange(array.shape[axis_at]) // (array.shape[axis_at] // parts)).reshape((-1,) + (1,) * (array.ndim - 1 - axis_at))

    near = jax.random.permutation(key, parts)[block_of(target)]
    second = (block_of(target) + parts // 2) % parts
    return jnp.where((block_of(source) == near) | (block_of(source) == second), factor * array, array)


def shard_levels(rng, dims, split, low, top_value):
    def one(dim, blocks):
        heights = jax.random.uniform(jax.random.fold_in(jax.random.fold_in(rng, 6), dim), (blocks,), jnp.float32, low / len(split), top_value / len(split))
        return jnp.repeat(jnp.exp(heights), dims[dim] // blocks).reshape((-1,) + (1,) * (len(dims) - dim - 1))

    factor_of = one(*split[0])
    for cut in split[1:]:
        factor_of = factor_of * one(*cut)
    return factor_of


def centred(own_key, dims, spread, reach, cuts=(), dtype=jnp.bfloat16):
    values = jax.random.normal(own_key, dims, jnp.float32) * spread
    if len(cuts) > 0:
        values = shard_levels(own_key, dims, cuts, -0.22, 0.18) * values
    return jnp.clip(values, min=-reach, max=reach).astype(dtype)


def bell_draw_with(stream_key, dims, spread, bound, split, heavy, held_as=jnp.bfloat16):
    array = spread * jax.random.normal(stream_key, dims, jnp.float32)
    if split:
        array = array * shard_levels(stream_key, dims, split, -0.22, 0.18)
    return jnp.clip(with_spikes(array, jax.random.fold_in(stream_key, 3), *heavy), -bound, bound).astype(held_as)


def setup_inputs(seed: int = 0) -> dict:
    key_list = jax.random.split(jax.random.key(seed), 3)
    grad_out = bell_draw_with(key_list[0], (TOKENS, D), 1.0, 6.0, ((0, 8), (1, 4)), (1, 0, 8, 2.0))
    weight = centred(key_list[1], (FF, D), D ** -0.5, 0.0625, ((0, 8), (1, 4)))
    return {"grad_out": grad_out, "weight": weight}


def reference(grad_out, weight):
    blocks = weight.reshape(8, FF // 8, D)

    def one_block(block):
        return jnp.dot(grad_out, block.T, preferred_element_type=jnp.float32).astype(jnp.bfloat16)

    result = lax.map(one_block, blocks)
    return jnp.transpose(result, (1, 0, 2)).reshape(TOKENS, FF)
```

```python
import jax
import jax.numpy as jnp
from jax import lax
from jax.sharding import PartitionSpec as P

CHUNKS = 4
LIFT = 2.0**40
TOP = 240.0


def contract(rows_block, weight):
    return lax.dot_general(
        rows_block, weight, (((1,), (1,)), ((), ())), preferred_element_type=jnp.float32
    )


def gather_tokens(block, cols):
    me = lax.axis_index("col")
    tokens = block.shape[0]
    pairs = cols // 2
    group, core = me // 2, me % 2

    def step(value, sources, by):
        return lax.ppermute(value, "col", [(2 * g + c, 2 * (g + by) + c) for g in sources for c in (0, 1)])

    def swap(value, groups):
        return lax.ppermute(value, "col", [(2 * g + c, 2 * g + 1 - c) for g in groups for c in (0, 1)])

    up, down = {0: block}, {0: block}
    up_pair, down_pair = {}, {}
    other = swap(block, range(pairs))
    for d in range(1, pairs):
        up[d] = step(up[d - 1], range(d - 1, pairs - 1), 1)
        down[d] = step(down[d - 1], range(1, pairs - d + 1), -1)
        up_pair[d] = swap(up[d], range(d, pairs))
        down_pair[d] = swap(down[d], range(0, pairs - d))
    whole = jnp.zeros((cols * tokens, block.shape[1]), block.dtype)

    def put(whole, own, twin, at):
        first = jnp.where(core == 0, own, twin)
        second = jnp.where(core == 0, twin, own)
        return lax.dynamic_update_slice(whole, jnp.concatenate([first, second], 0), (at * 2 * tokens, 0))

    whole = put(whole, block, other, group)
    for d in range(1, pairs):
        below = group >= d
        own = jnp.where(below, up[d], down[pairs - d])
        twin = jnp.where(below, up_pair[d], down_pair[pairs - d])
        whole = put(whole, own, twin, (group - d + pairs) % pairs)
    return whole


def norm_bound(value):
    lifted = value.astype(jnp.float32) * LIFT
    return jnp.sqrt(jnp.max(jnp.sum(lifted * lifted, axis=1, keepdims=True), axis=0, keepdims=True))


def encode(value, bound):
    scaled = value * (TOP / bound)
    return (scaled * jnp.abs(scaled)).astype(jnp.float16)


def decode(code, bound):
    code = code.astype(jnp.float32)
    return code * lax.rsqrt(jnp.maximum(jnp.abs(code), 1e-9)) * (bound / TOP)


def exchange(value, distance, rows):
    return lax.ppermute(value, "row", [(i, i ^ distance) for i in range(rows)])


def bounds_of(bound, order, rows):
    steps = []
    for distance in order:
        arriving = exchange(bound, distance, rows)
        steps.append((bound, arriving))
        bound = bound + arriving
    return steps


def halve(part, order, bounds, rows):
    tokens = part.shape[0] // rows
    held = {k: part[k * tokens : (k + 1) * tokens] for k in range(rows)}
    for distance, (sent_bound, got_bound) in zip(order, bounds):
        moved = sorted(k for k in held if k & distance)
        got = [exchange(encode(held[k], sent_bound), distance, rows) for k in moved]
        for k, code in zip(moved, got):
            held[k ^ distance] = held[k ^ distance] + decode(code, got_bound)
            del held[k]
    return held[0]


def solution(mesh):
    rows, cols = mesh.shape["row"], mesh.shape["col"]
    bits = [1 << b for b in range((rows - 1).bit_length())]

    def local(grad_out, weight):
        me = lax.axis_index("row")
        everyone = gather_tokens(grad_out, cols)
        tokens = everyone.shape[0] // rows
        hidden = weight.shape[0]
        chunks = CHUNKS
        while hidden % chunks:
            chunks -= 1
        width = hidden // chunks
        lhs = jnp.concatenate(
            [lax.dynamic_slice_in_dim(everyone, (me ^ k) * tokens, tokens, 0) for k in range(rows)], 0
        )
        bound = (norm_bound(everyone) / LIFT) * (norm_bound(weight) / LIFT)
        bound = jnp.maximum(bound, 1e-36)
        orders = [bits[t:] + bits[:t] for t in range(len(bits))]
        bounds = [bounds_of(bound, order, rows) for order in orders]
        outs = []
        for i in range(chunks):
            part = contract(lhs, weight[i * width : (i + 1) * width])
            turn = i % len(orders)
            outs.append(halve(part, orders[turn], bounds[turn], rows).astype(jnp.bfloat16))
        return jnp.concatenate(outs, 1)

    return jax.shard_map(
        local,
        mesh=mesh,
        in_specs=(P("col", "row"), P("col", "row")),
        out_specs=P("row", "col"),
        check_vma=False,
    )
```

```python
import jax
import jax.numpy as jnp
from jax import lax
from jax.sharding import PartitionSpec as P

CHUNKS = 4
LIFT = 2.0**40
TOP = 240.0


def contract(rows_block, weight):
    return lax.dot_general(
        rows_block, weight, (((1,), (1,)), ((), ())), preferred_element_type=jnp.float32
    )


def gather_tokens(block, cols):
    me = lax.axis_index("col")
    tokens = block.shape[0]
    pairs = cols // 2
    group, core = me // 2, me % 2

    def step(value, sources, by):
        return lax.ppermute(value, "col", [(2 * g + c, 2 * (g + by) + c) for g in sources for c in (0, 1)])

    def swap(value, groups):
        return lax.ppermute(value, "col", [(2 * g + c, 2 * g + 1 - c) for g in groups for c in (0, 1)])

    if pairs == 4:
        everyone = range(pairs)
        far = lax.ppermute(
            block, "col", [(2 * g + c, 2 * (g ^ 2) + c) for g in everyone for c in (0, 1)]
        )
        rise = step(block, range(0, 3), 1)
        fall = step(block, range(1, 4), -1)
        other = swap(block, everyone)
        ends = lax.ppermute(
            far, "col", [(2 * g + c, 2 * h + c) for g, h in ((1, 0), (2, 3)) for c in (0, 1)]
        )
        far_pair = swap(far, everyone)
        below = jnp.where(group == 0, ends, rise)
        above = jnp.where(group == 3, ends, fall)
        near_pair = swap(jnp.concatenate([below, above], 0), everyone)
        own = {1: below, 2: far, 3: above}
        twin = {1: near_pair[:tokens], 2: far_pair, 3: near_pair[tokens:]}
    else:
        up, down = {0: block}, {0: block}
        up_pair, down_pair = {}, {}
        other = swap(block, range(pairs))
        for d in range(1, pairs):
            up[d] = step(up[d - 1], range(d - 1, pairs - 1), 1)
            down[d] = step(down[d - 1], range(1, pairs - d + 1), -1)
            up_pair[d] = swap(up[d], range(d, pairs))
            down_pair[d] = swap(down[d], range(0, pairs - d))
        own = {d: jnp.where(group >= d, up[d], down[pairs - d]) for d in range(1, pairs)}
        twin = {d: jnp.where(group >= d, up_pair[d], down_pair[pairs - d]) for d in range(1, pairs)}
    whole = jnp.zeros((cols * tokens, block.shape[1]), block.dtype)

    def put(whole, own, twin, at):
        first = jnp.where(core == 0, own, twin)
        second = jnp.where(core == 0, twin, own)
        return lax.dynamic_update_slice(whole, jnp.concatenate([first, second], 0), (at * 2 * tokens, 0))

    whole = put(whole, block, other, group)
    for d in range(1, pairs):
        whole = put(whole, own[d], twin[d], (group - d + pairs) % pairs)
    return whole


def norm_bound(value):
    lifted = value.astype(jnp.float32) * LIFT
    return jnp.sqrt(jnp.max(jnp.sum(lifted * lifted, axis=1, keepdims=True), axis=0, keepdims=True))


def encode(value, level):
    scaled = value * (TOP / jnp.exp2(level))
    return (scaled * jnp.abs(scaled)).astype(jnp.float16)


def decode(code, level):
    code = code.astype(jnp.float32)
    return code * lax.rsqrt(jnp.maximum(jnp.abs(code), 1e-9)) * (jnp.exp2(level) / TOP)


def exchange(value, distance, rows):
    return lax.ppermute(value, "row", [(i, i ^ distance) for i in range(rows)])


def halve(part, order, level, known, rows, hold):
    tokens = part.shape[0] // rows
    held = {k: part[k * tokens : (k + 1) * tokens] for k in range(rows)}
    for distance in order:
        moved = sorted((k for k in held if k & distance), reverse=True)
        fresh = (distance, "got") not in known
        if fresh:
            known[distance, "sent"] = level
        level = known[distance, "sent"]
        sent = [encode(held[k], level) for k in moved]
        if fresh:
            extra = jnp.broadcast_to(level.astype(jnp.float16), (16, part.shape[1]))
            sent[0] = jnp.concatenate([sent[0], extra], 0)
        if distance == order[0]:
            sent = hold(sent)
        got = [exchange(code, distance, rows) for code in sent]
        if fresh:
            known[distance, "got"] = got[0][tokens : tokens + 1, :1].astype(jnp.float32)
        got = {k: code[:tokens] for k, code in zip(moved, got)}
        for k in moved:
            held[k ^ distance] = held[k ^ distance] + decode(got[k], known[distance, "got"])
            del held[k]
        level = jnp.maximum(level, known[distance, "got"]) + 1.0
    return held[0]


def solution(mesh):
    rows, cols = mesh.shape["row"], mesh.shape["col"]
    bits = [1 << b for b in range((rows - 1).bit_length())]

    def local(grad_out, weight):
        me = lax.axis_index("row")
        everyone = gather_tokens(grad_out, cols)
        tokens = everyone.shape[0] // rows
        hidden = weight.shape[0]
        chunks = CHUNKS
        while hidden % chunks:
            chunks -= 1
        width = hidden // chunks
        lhs = jnp.concatenate(
            [lax.dynamic_slice_in_dim(everyone, (me ^ k) * tokens, tokens, 0) for k in range(rows)], 0
        )
        bound = (norm_bound(everyone) / LIFT) * (norm_bound(weight) / LIFT)
        level = jnp.ceil(jnp.log2(jnp.maximum(bound, 1e-35)) + 0.01)
        orders = [bits[t:] + bits[:t] for t in range(len(bits))]
        known = [{} for _ in orders]
        waiting = [lhs]

        def hold(codes):
            waiting[0], *codes = lax.optimization_barrier((waiting[0], *codes))
            return codes

        outs = []
        for i in range(chunks):
            part = contract(waiting[0], weight[i * width : (i + 1) * width])
            turn = i % len(orders)
            outs.append(halve(part, orders[turn], level, known[turn], rows, hold).astype(jnp.bfloat16))
        return jnp.concatenate(outs, 1)

    return jax.shard_map(
        local,
        mesh=mesh,
        in_specs=(P("col", "row"), P("col", "row")),
        out_specs=P("row", "col"),
        check_vma=False,
    )
```
